32 devices in a mesh: slab: 8 (over z, x), sub: 4 (over y, core).
Axes of the slice: x: 2, y: 2, z: 4, core: 2. Of those that a mesh axis runs over, the one named last changes fastest.
Arguments:
- values: float32 [768, 2, 128, 256], P(('slab', 'sub')), may hold values from -0.25 to 0.25
- block_ids: int32 [768, 2], P(('slab', 'sub')), may hold values from 0 to 383, as said below
- tile_counts: int32 [8, 4], P('slab', 'sub'), may hold values from 8 to 24, as said below
- right_side: float32 [768, 128], P(('slab', 'sub')), may hold values from -18 to 18
Outputs:
- solution: float32 [384, 256], P(('slab', 'sub'))
- residual: float32 [768, 128], P(('slab', 'sub'))
The draws below stay inside these ranges and needn't reach their ends.
Inputs may be any that keep to these rules, and one draw needn't show every extreme that they name: `block_ids`: every block id names a node block held by a device of the row tile's own slab or of a slab one index of slab away; the first coupled block of each tile lies in its own slab. Block b is held by device b div 12. `tile_counts`: some device has all 24 slots live in every draw.
All inputs are finite; a program needn't handle non-finite values.
Results may differ from the reference program's by a relative error of at most 0.0003.
Values sent between devices are 32-bit elements; how exact they have to be, the bound alone decides.
A program may use at most 64 MiB of HBM per device.

```python
import jax
import jax.numpy as jnp
from jax import lax

BLOCK = 256
TILE_ROWS = 128
COUPLED = 2
ITERS = 4
TILES_DEV = 24
NB_DEV = 12
TILES = 768
NBLOCKS = 384
N_SLAB = 8
N_SUB = 4


def draw_block_ids(key, part):
    tile_slab = jnp.arange(TILES, dtype=jnp.int32) // TILES_DEV // N_SUB
    offset = jax.random.randint(jax.random.fold_in(key, 11), (TILES, COUPLED), -1, 2)
    first_slot = jnp.arange(COUPLED, dtype=jnp.int32)[None, :] == 0
    offset = jnp.where(first_slot, 0, offset)
    other_slab = jnp.clip(tile_slab[:, None] + offset, 0, N_SLAB - 1)
    owner_sub = jax.random.randint(jax.random.fold_in(key, 12), (TILES, COUPLED), 0, N_SUB)
    slot_index = jax.random.randint(jax.random.fold_in(key, 13), (TILES, COUPLED), 0, NB_DEV)
    return ((other_slab * N_SUB + owner_sub) * NB_DEV + slot_index).astype(jnp.int32)


def draw_tile_counts(key, part):
    lowest = TILES_DEV // 3
    counts = jax.random.randint(jax.random.fold_in(key, 21), (N_SLAB * N_SUB,), lowest, TILES_DEV + 1)
    fuller = jax.random.randint(jax.random.fold_in(key, 22), (), 0, N_SLAB * N_SUB)
    counts = jnp.where(jnp.arange(N_SLAB * N_SUB, dtype=jnp.int32) == fuller, TILES_DEV, counts)
    return counts.reshape(N_SLAB, N_SUB).astype(jnp.int32)


def draw_right_side(key, part):
    position = jnp.arange(TILES, dtype=jnp.float32) / max(TILES - 1, 1)
    base = jnp.clip(jax.random.normal(jax.random.fold_in(key, 32), (TILES, TILE_ROWS), jnp.float32), -6.0, 6.0)
    rising = 1.0 + 2.0 * position
    return (base * rising[:, None]).astype(jnp.float32)


def steps_of(stream_key, extent, shards, smallest, top_value):
    level = 1.0
    for dim, parts in shards:
        heights = jax.random.uniform(jax.random.fold_in(jax.random.fold_in(stream_key, 6), dim), (parts,), jnp.float32, smallest / len(shards), top_value / len(shards))
        level = level * jnp.repeat(jnp.exp(heights), extent[dim] // parts).reshape((-1,) + (1,) * (len(extent) - 1 - dim))
    return level


def bell_draw(key, extent, width, reach, split=(), held_as=jnp.bfloat16):
    entries = jax.random.normal(key, extent, jnp.float32) * width
    if len(split) > 0:
        entries = steps_of(key, extent, split, -0.22, 0.18) * entries
    return jnp.clip(entries, min=-reach, max=reach).astype(held_as)


def setup_inputs(seed: int = 0) -> dict:
    key_list = jax.random.split(jax.random.key(seed), 5)
    return {
        "values": bell_draw(key_list[0], (TILES, COUPLED, TILE_ROWS, BLOCK), (COUPLED * BLOCK) ** -0.5, 0.25, ((0, 32),), jnp.float32),
        "block_ids": draw_block_ids(jax.random.fold_in(key_list[4], 71), 0),
        "tile_counts": draw_tile_counts(jax.random.fold_in(key_list[4], 71), 0),
        "right_side": draw_right_side(jax.random.fold_in(key_list[4], 71), 0),
    }


precise = lax.Precision.HIGHEST


def live_mask(tile_counts):
    position = jnp.arange(TILES, dtype=jnp.int32)
    owner_dev = (position // TILES_DEV).astype(jnp.int32)
    limit = tile_counts.reshape(-1)[owner_dev]
    return ((position % TILES_DEV) < limit).astype(jnp.float32)


def forward(values, block_ids, live_tiles, field):
    picked = field[block_ids]
    image = jnp.einsum("tkij,tkj->ti", values, picked, precision=precise)
    return image * live_tiles[:, None]


def backward(values, block_ids, rows):
    terms = jnp.einsum("tkij,ti->tkj", values, rows, precision=precise)
    return jax.ops.segment_sum(terms.reshape(-1, BLOCK), block_ids.reshape(-1), num_segments=NBLOCKS)


def reference(values, block_ids, tile_counts, right_side):
    live_tiles = live_mask(tile_counts)
    squares = jnp.einsum("tkij,tkij->tkj", values, values, precision=precise) * live_tiles[:, None, None]
    col_squares = jax.ops.segment_sum(squares.reshape(-1, BLOCK), block_ids.reshape(-1), num_segments=NBLOCKS)
    jacobi = 1.0 / (1.0 + col_squares)
    solution = jnp.zeros((NBLOCKS, BLOCK), jnp.float32)
    residual = right_side * live_tiles[:, None]
    normal_res = backward(values, block_ids, residual)
    scaled = jacobi * normal_res
    direction = scaled
    rho_now = jnp.sum(normal_res * scaled)
    for iteration in range(ITERS):
        image = forward(values, block_ids, live_tiles, direction)
        step_size = rho_now / jnp.sum(image * image)
        solution = solution + step_size * direction
        residual = residual - step_size * image
        normal_res = backward(values, block_ids, residual)
        scaled = jacobi * normal_res
        rho_next = jnp.sum(normal_res * scaled)
        direction = scaled + (rho_next / rho_now) * direction
        rho_now = rho_next
    return (solution, residual)
```

```python
import functools

import jax
import jax.numpy as jnp
from jax import lax
from jax.experimental import pallas as pl
from jax.experimental.pallas import tpu as pltpu
from jax.sharding import PartitionSpec as P

ITERS = 4
NB_DEV = 12
LANES = 128
MESH = pl.DeviceIdType.MESH


def round_up(size, unit):
    return -(-size // unit) * unit


def kernel(
    n_slab,
    n_sub,
    values_hbm,
    ids_smem,
    counts_smem,
    right_ref,
    solution_ref,
    residual_ref,
    values,
    wid,
    turned,
    selector,
    terms,
    squares,
    image_cols,
    image_rows,
    first_out,
    first_in,
    part_out,
    part_in,
    field_out,
    field_in,
    scaled_win,
    direction_win,
    scal1,
    scal2,
    load_sem,
    first_send,
    first_recv,
    part_send,
    part_recv,
    field_send,
    field_recv,
    scal1_send,
    scal1_recv,
    scal2_send,
    scal2_recv,
):
    tiles, coupled, rows, block = values.shape
    halves = block // LANES
    held = NB_DEV * halves
    n = n_slab * n_sub
    window = 3 * n_sub * held
    f32 = jnp.float32
    slab = lax.axis_index("slab")
    sub = lax.axis_index("sub")
    me = slab * n_sub + sub

    for t in range(tiles):
        pltpu.make_async_copy(values_hbm.at[t], values.at[t], load_sem.at[t]).start()

    def other(j):
        target = lax.rem(me + j, n)
        return (lax.div(target, n_sub), lax.rem(target, n_sub))

    barrier = pltpu.get_barrier_semaphore()

    @pl.loop(1, n)
    def _(j):
        pl.semaphore_signal(barrier, inc=1, device_id=other(j), device_id_type=MESH)

    turned[...] = jnp.zeros_like(turned)
    terms[...] = jnp.zeros_like(terms)
    squares[...] = jnp.zeros_like(squares)
    lane_ids = lax.broadcasted_iota(jnp.int32, (1, turned.shape[1]), 1)

    @pl.loop(0, tiles)
    def _(t):
        for k in range(coupled):
            b = ids_smem[t, k]
            owner = lax.div(b, NB_DEV)
            rel = jnp.clip(lax.div(owner, n_sub) - slab + 1, 0, 2)
            row = (rel * n_sub + lax.rem(owner, n_sub)) * held + lax.rem(b, NB_DEV)
            wid[t, k] = row
            for h in range(halves):
                hot = (lane_ids == row + h * NB_DEV).astype(f32)
                turned[pl.ds((k * halves + h) * tiles + t, 1), :] = hot

    selector[...] = turned[...].T.astype(jnp.bfloat16)

    missing = ((slab == 0, 0, 1), (slab == n_slab - 1, 2, -1))
    for absent, rel, delta in missing:

        @pl.when(absent)
        def _(rel=rel, delta=delta):
            low = (delta + 1) * n_sub
            first_in[low : low + n_sub] = jnp.zeros((n_sub,) + first_in.shape[1:], f32)
            for it in range(part_in.shape[0]):
                part_in[it, low : low + n_sub] = jnp.zeros((n_sub,) + part_in.shape[2:], f32)
            for it in range(field_in.shape[0]):
                field_in[it, rel] = jnp.zeros(field_in.shape[2:], f32)

    def live(t):
        return jnp.where(t < counts_smem[0, 0], 1.0, 0.0).astype(f32)

    eye = (
        lax.broadcasted_iota(jnp.int32, (rows, LANES), 0)
        == lax.broadcasted_iota(jnp.int32, (rows, LANES), 1)
    ).astype(f32)

    def half(h):
        return slice(h * LANES, (h + 1) * LANES)

    def term_row(k, h, t):
        return pl.ds((k * halves + h) * tiles + t, 1)

    def scatter(term_refs):
        cut = []
        for ref in term_refs:
            rest = ref[...]
            for _ in range(3):
                piece = rest.astype(jnp.bfloat16)
                cut.append(piece)
                rest = rest - piece.astype(f32)
        spread = jnp.dot(
            selector[...], jnp.concatenate(cut, axis=1), preferred_element_type=f32
        )
        outs = []
        for i in range(len(term_refs)):
            a, b, c = (spread[:window, half(3 * i + j)] for j in range(3))
            outs.append((a + (b + c)).reshape(3, n_sub, held, LANES))
        return outs

    def partners():
        for ds in (1, -1, 0):
            for step in range(n_sub):
                if ds == 0 and step == 0:
                    continue
                exists = None
                if ds:
                    exists = slab + ds >= 0 if ds < 0 else slab + ds < n_slab
                source_exists = None
                if ds:
                    source_exists = slab - ds >= 0 if ds > 0 else slab - ds < n_slab
                yield ds, step, exists, source_exists

    def guarded(cond, act):
        if cond is None:
            act()
        else:
            pl.when(cond)(act)

    def part_copy(out_ref, in_ref, send, recv, ds, step):
        target = lax.rem(sub + step, n_sub)
        slot = (ds + 1) * n_sub + step
        return pltpu.make_async_remote_copy(
            src_ref=out_ref.at[ds + 1, target],
            dst_ref=in_ref.at[slot],
            send_sem=send.at[slot],
            recv_sem=recv.at[slot],
            device_id=(slab + ds, target),
            device_id_type=MESH,
        )

    def field_copy(it, ds, step):
        target = lax.rem(sub + step, n_sub)
        slot = (ds + 1) * n_sub + step
        return pltpu.make_async_remote_copy(
            src_ref=field_out.at[it],
            dst_ref=field_in.at[it, 1 - ds, sub],
            send_sem=field_send.at[it, slot],
            recv_sem=field_recv.at[it, slot],
            device_id=(slab + ds, target),
            device_id_type=MESH,
        )

    def start_all(copy):
        for ds, step, exists, _ in partners():
            guarded(exists, lambda ds=ds, step=step: copy(ds, step).start())

    def wait_recv_all(copy):
        for ds, step, _, source in partners():
            guarded(source, lambda ds=ds, step=step: copy(ds, step).wait_recv())

    def wait_send_all(copy):
        for ds, step, exists, _ in partners():
            guarded(exists, lambda ds=ds, step=step: copy(ds, step).wait_send())

    def scal_copy(ref, send, recv, it, j):
        return pltpu.make_async_remote_copy(
            src_ref=ref.at[it, me],
            dst_ref=ref.at[it, me],
            send_sem=send.at[it],
            recv_sem=recv.at[it],
            device_id=other(j),
            device_id_type=MESH,
        )

    def scal_start(ref, send, recv, it):
        @pl.loop(1, n)
        def _(j):
            scal_copy(ref, send, recv, it, j).start()

    def scal_all(ref, send, recv, it):
        rest = ref.at[it, pl.ds(0, n - 1)]
        return pltpu.make_async_remote_copy(
            src_ref=rest,
            dst_ref=rest,
            send_sem=send.at[it],
            recv_sem=recv.at[it],
            device_id=other(1),
            device_id_type=MESH,
        )

    def total(x):
        return jnp.sum(jnp.sum(x, axis=0, keepdims=True), axis=1, keepdims=True)

    @pl.loop(0, tiles)
    def _(t):
        pltpu.make_async_copy(values_hbm.at[t], values.at[t], load_sem.at[t]).wait()
        alive = live(t)
        cols = jnp.sum(eye * (right_ref[pl.ds(t, 1), :] * alive), axis=1, keepdims=True)
        cols = jnp.broadcast_to(cols, (rows, LANES))
        for k in range(coupled):
            for h in range(halves):
                a = values[t, k, :, half(h)]
                terms[term_row(k, h, t), :] = jnp.sum(a * cols, axis=0, keepdims=True)
                squares[term_row(k, h, t), :] = (
                    jnp.sum(a * a, axis=0, keepdims=True) * alive
                )
        residual_ref[pl.ds(t, 1), :] = right_ref[pl.ds(t, 1), :] * alive

    pieces = scatter((terms, squares))
    for i in range(2):
        first_out[:, :, i] = pieces[i]
    pl.semaphore_wait(barrier, n - 1)
    first_copy = functools.partial(part_copy, first_out, first_in, first_send, first_recv)
    start_all(first_copy)
    wait_recv_all(first_copy)
    sums = first_out[1, sub]
    for slot in range(3 * n_sub):
        if slot != n_sub:
            sums = sums + first_in[slot]
    normal_res = sums[0]
    jacobi = 1.0 / (1.0 + sums[1])
    scaled = jacobi * normal_res
    field_out[0] = scaled
    rho_part = total(normal_res * scaled)
    scal2[0, me] = jnp.broadcast_to(rho_part, (2, LANES))
    scal_start(scal2, scal2_send, scal2_recv, 0)
    start_all(functools.partial(field_copy, 0))
    field_in[0, 1, sub] = scaled
    wait_recv_all(functools.partial(field_copy, 0))
    scaled_win[...] = field_in[0].reshape(window, LANES)
    direction_win[...] = scaled_win[...]
    scal_all(scal2, scal2_send, scal2_recv, 0).wait_recv()
    rho_now = jnp.sum(scal2[0], axis=0)[0:1]

    answer = jnp.zeros((held, LANES), f32)
    own_rows = pl.ds(pl.multiple_of((n_sub + sub) * held, 8), held)
    for it in range(ITERS):
        last = it == ITERS - 1

        def tile_pass(t, norm):
            alive = live(t)
            m = None
            for k in range(coupled):
                for h in range(halves):
                    picked = direction_win[pl.ds(wid[t, k] + h * NB_DEV, 1), :] * alive
                    product = values[t, k, :, half(h)] * picked
                    m = product if m is None else m + product
            image = jnp.broadcast_to(jnp.sum(m, axis=1, keepdims=True), (rows, LANES))
            image_cols[t] = image
            if not last:
                for k in range(coupled):
                    for h in range(halves):
                        terms[term_row(k, h, t), :] = jnp.sum(
                            values[t, k, :, half(h)] * image, axis=0, keepdims=True
                        )
            return norm + jnp.sum(image * image, axis=0, keepdims=True)

        norm = lax.fori_loop(0, tiles, tile_pass, jnp.zeros((1, LANES), f32), unroll=2)
        scal1[it, me] = norm
        if not last:
            part_out[it] = scatter((terms,))[0]
            out_copy = functools.partial(
                part_copy, part_out.at[it], part_in.at[it], part_send.at[it], part_recv.at[it]
            )
            start_all(out_copy)
        scal_start(scal1, scal1_send, scal1_recv, it)

        @pl.loop(0, tiles)
        def _(t):
            image_rows[pl.ds(t, 1), :] = jnp.sum(image_cols[t] * eye, axis=0, keepdims=True)

        if not last:
            wait_recv_all(out_copy)
            back = part_out[it, 1, sub]
            for slot in range(3 * n_sub):
                if slot != n_sub:
                    back = back + part_in[it, slot]
            back_scaled = jacobi * back
            field_out[it + 1] = back_scaled
            scal2[it + 1, me, 0:1] = jnp.broadcast_to(total(scaled * back), (1, LANES))
            scal2[it + 1, me, 1:2] = jnp.broadcast_to(total(back * back_scaled), (1, LANES))
            scal_start(scal2, scal2_send, scal2_recv, it + 1)
            start_all(functools.partial(field_copy, it + 1))
            field_in[it + 1, 1, sub] = back_scaled
        scal_all(scal1, scal1_send, scal1_recv, it).wait_recv()
        step_size = rho_now / jnp.sum(scal1[it], axis=0)
        answer = answer + step_size * direction_win[own_rows, :]
        residual_ref[...] = residual_ref[...] - step_size * image_rows[...]
        if not last:
            scaled = scaled - step_size * back_scaled
            wait_recv_all(functools.partial(field_copy, it + 1))
            scaled_win[...] = scaled_win[...] - step_size * field_in[it + 1].reshape(window, LANES)
            scal_all(scal2, scal2_send, scal2_recv, it + 1).wait_recv()
            both = jnp.sum(scal2[it + 1], axis=0)
            rho_next = rho_now - 2.0 * step_size * both[0:1] + step_size * step_size * both[1:2]
            direction_win[...] = scaled_win[...] + (rho_next / rho_now) * direction_win[...]
            rho_now = rho_next

    for h in range(halves):
        solution_ref[:, half(h)] = answer[h * NB_DEV : (h + 1) * NB_DEV]

    wait_send_all(first_copy)
    for it in range(ITERS):
        wait_send_all(functools.partial(field_copy, it))
        scal_all(scal1, scal1_send, scal1_recv, it).wait_send()
        scal_all(scal2, scal2_send, scal2_recv, it).wait_send()
        if it < ITERS - 1:
            wait_send_all(
                functools.partial(
                    part_copy, part_out.at[it], part_in.at[it], part_send.at[it], part_recv.at[it]
                )
            )


def per_device(n_slab, n_sub, values, block_ids, tile_counts, right_side):
    tiles, coupled, rows, block = values.shape
    halves = block // LANES
    held = NB_DEV * halves
    n = n_slab * n_sub
    slots = 3 * n_sub
    window = slots * held
    n_terms = round_up(tiles * coupled * halves, LANES)
    n_window = round_up(window, LANES)
    f32 = jnp.float32
    vmem = pltpu.VMEM
    dma = pltpu.SemaphoreType.DMA
    whole = pl.BlockSpec(memory_space=pltpu.VMEM)
    scalars = pl.BlockSpec(memory_space=pltpu.SMEM)
    return pl.pallas_call(
        functools.partial(kernel, n_slab, n_sub),
        out_shape=(
            jax.ShapeDtypeStruct((NB_DEV, block), f32),
            jax.ShapeDtypeStruct((tiles, rows), f32),
        ),
        in_specs=[pl.BlockSpec(memory_space=pl.ANY), scalars, scalars, whole],
        out_specs=(whole, whole),
        scratch_shapes=[
            vmem(values.shape, f32),
            pltpu.SMEM((tiles, coupled), jnp.int32),
            vmem((n_terms, n_window), f32),
            vmem((n_window, n_terms), jnp.bfloat16),
            vmem((n_terms, LANES), f32),
            vmem((n_terms, LANES), f32),
            vmem((tiles, rows, LANES), f32),
            vmem((tiles, LANES), f32),
            vmem((3, n_sub, 2, held, LANES), f32),
            vmem((slots, 2, held, LANES), f32),
            vmem((ITERS - 1, 3, n_sub, held, LANES), f32),
            vmem((ITERS - 1, slots, held, LANES), f32),
            vmem((ITERS, held, LANES), f32),
            vmem((ITERS, 3, n_sub, held, LANES), f32),
            vmem((window, LANES), f32),
            vmem((window, LANES), f32),
            vmem((ITERS, n, 1, LANES), f32),
            vmem((ITERS, n, 2, LANES), f32),
            dma((tiles,)),
            dma((slots,)),
            dma((slots,)),
            dma((ITERS - 1, slots)),
            dma((ITERS - 1, slots)),
            dma((ITERS, slots)),
            dma((ITERS, slots)),
            dma((ITERS,)),
            dma((ITERS,)),
            dma((ITERS,)),
            dma((ITERS,)),
        ],
        compiler_params=pltpu.CompilerParams(
            collective_id=0, has_side_effects=True, vmem_limit_bytes=48 * 1024 * 1024
        ),
    )(values, block_ids, tile_counts, right_side)


def solution(mesh):
    in_specs = (
        P(("slab", "sub"), None, None, None),
        P(("slab", "sub"), None),
        P("slab", "sub"),
        P(("slab", "sub"), None),
    )
    out_specs = (P(("slab", "sub"), None), P(("slab", "sub"), None))
    return jax.shard_map(
        functools.partial(per_device, mesh.shape["slab"], mesh.shape["sub"]),
        mesh=mesh,
        in_specs=in_specs,
        out_specs=out_specs,
        check_vma=False,
    )
```

```python
import functools

import jax
import jax.numpy as jnp
from jax import lax
from jax.experimental import pallas as pl
from jax.experimental.pallas import tpu as pltpu
from jax.sharding import PartitionSpec as P

ITERS = 4
NB_DEV = 12
LANES = 128
MESH = pl.DeviceIdType.MESH


def round_up(size, unit):
    return -(-size // unit) * unit


def kernel(
    n_slab,
    n_sub,
    values_hbm,
    ids_hbm,
    counts_hbm,
    right_hbm,
    solution_ref,
    residual_ref,
    values,
    wid,
    turned,
    selector,
    terms,
    squares,
    image_cols,
    image_rows,
    first_out,
    first_in,
    part_out,
    part_in,
    field_out,
    field_in,
    scaled_win,
    direction_win,
    scal1,
    scal2,
    ids_smem,
    counts_smem,
    right_ref,
    small_sem,
    load_sem,
    first_send,
    first_recv,
    part_send,
    part_recv,
    field_send,
    field_recv,
    scal1_send,
    scal1_recv,
    scal2_send,
    scal2_recv,
):
    tiles, coupled, rows, block = values.shape
    halves = block // LANES
    held = NB_DEV * halves
    n = n_slab * n_sub
    window = 3 * n_sub * held
    f32 = jnp.float32
    slab = lax.axis_index("slab")
    sub = lax.axis_index("sub")
    me = slab * n_sub + sub

    def keeper(s):
        return s + 1 - 2 * lax.rem(s, 2) if n_slab % 2 == 0 else s

    kept = keeper(slab)

    small = [
        pltpu.make_async_copy(src, dst, small_sem.at[i])
        for i, (src, dst) in enumerate(
            ((ids_hbm, ids_smem), (counts_hbm, counts_smem), (right_hbm, right_ref))
        )
    ]
    for copy in small:
        copy.start()
    for t in range(tiles):
        pltpu.make_async_copy(values_hbm.at[t], values.at[t], load_sem.at[t]).start()

    def other(j):
        target = lax.rem(me + j, n)
        return (lax.div(target, n_sub), lax.rem(target, n_sub))

    barrier = pltpu.get_barrier_semaphore()

    @pl.loop(1, n)
    def _(j):
        pl.semaphore_signal(barrier, inc=1, device_id=other(j), device_id_type=MESH)

    for copy in small:
        copy.wait()

    turned[...] = jnp.zeros_like(turned)
    terms[...] = jnp.zeros_like(terms)
    squares[...] = jnp.zeros_like(squares)
    lane_ids = lax.broadcasted_iota(jnp.int32, (1, turned.shape[1]), 1)

    @pl.loop(0, tiles)
    def _(t):
        for k in range(coupled):
            b = ids_smem[t, k]
            owner = lax.div(b, NB_DEV)
            rel = jnp.clip(lax.div(owner, n_sub) - slab + 1, 0, 2)
            row = (rel * n_sub + lax.rem(owner, n_sub)) * held + lax.rem(b, NB_DEV)
            wid[t, k] = row
            for h in range(halves):
                hot = (lane_ids == row + h * NB_DEV).astype(f32)
                turned[pl.ds((k * halves + h) * tiles + t, 1), :] = hot

    selector[...] = turned[...].T.astype(jnp.bfloat16)

    def blank_part(low):
        first_in[low : low + n_sub] = jnp.zeros((n_sub,) + first_in.shape[1:], f32)
        for it in range(part_in.shape[0]):
            part_in[it, low : low + n_sub] = jnp.zeros((n_sub,) + part_in.shape[2:], f32)

    def blank_field(rel):
        for it in range(field_in.shape[0]):
            field_in[it, rel] = jnp.zeros(field_in.shape[2:], f32)

    pl.when(kept == 0)(lambda: blank_part(2 * n_sub))
    pl.when(kept == n_slab - 1)(lambda: blank_part(0))
    pl.when(slab == 0)(lambda: blank_field(0))
    pl.when(slab == n_slab - 1)(lambda: blank_field(2))

    def live(t):
        return jnp.where(t < counts_smem[0, 0], 1.0, 0.0).astype(f32)

    eye = (
        lax.broadcasted_iota(jnp.int32, (rows, LANES), 0)
        == lax.broadcasted_iota(jnp.int32, (rows, LANES), 1)
    ).astype(f32)

    def half(h):
        return slice(h * LANES, (h + 1) * LANES)

    def term_row(k, h, t):
        return pl.ds((k * halves + h) * tiles + t, 1)

    def scatter(term_refs):
        cut = []
        for ref in term_refs:
            rest = ref[...]
            for _ in range(3):
                piece = rest.astype(jnp.bfloat16)
                cut.append(piece)
                rest = rest - piece.astype(f32)
        spread = jnp.dot(
            selector[...], jnp.concatenate(cut, axis=1), preferred_element_type=f32
        )
        outs = []
        for i in range(len(term_refs)):
            a, b, c = (spread[:window, half(3 * i + j)] for j in range(3))
            outs.append((a + (b + c)).reshape(3, n_sub, held, LANES))
        return outs

    def inside(s):
        return jnp.logical_and(s >= 0, s < n_slab)

    def each(act, scatters):
        for ds in (1, -1, 0):
            for step in range(n_sub):
                if scatters:
                    exists, far = inside(slab + ds), keeper(slab + ds)
                else:
                    exists, far = inside(kept - ds), kept - ds
                if step == 0:
                    exists = jnp.logical_and(exists, far != slab)
                pl.when(exists)(functools.partial(act, ds, step))

    def part_copy(out_ref, in_ref, send, recv, ds, step):
        target = lax.rem(sub + step, n_sub)
        slot = (ds + 1) * n_sub + step
        return pltpu.make_async_remote_copy(
            src_ref=out_ref.at[ds + 1, target],
            dst_ref=in_ref.at[slot],
            send_sem=send.at[slot],
            recv_sem=recv.at[slot],
            device_id=(keeper(slab + ds), target),
            device_id_type=MESH,
        )

    def field_copy(it, ds, step):
        target = lax.rem(sub + step, n_sub)
        slot = (ds + 1) * n_sub + step
        return pltpu.make_async_remote_copy(
            src_ref=field_out.at[it],
            dst_ref=field_in.at[it, ds + 1, sub],
            send_sem=field_send.at[it, slot],
            recv_sem=field_recv.at[it, slot],
            device_id=(kept - ds, target),
            device_id_type=MESH,
        )

    def start_all(copy, scatters):
        each(lambda ds, step: copy(ds, step).start(), scatters)

    def wait_recv_all(copy, scatters):
        each(lambda ds, step: copy(ds, step).wait_recv(), not scatters)

    def wait_send_all(copy, scatters):
        each(lambda ds, step: copy(ds, step).wait_send(), scatters)

    own_rel = kept - slab + 1
    own_slot = own_rel * n_sub

    def scal_copy(ref, send, recv, it, j):
        return pltpu.make_async_remote_copy(
            src_ref=ref.at[it, me],
            dst_ref=ref.at[it, me],
            send_sem=send.at[it],
            recv_sem=recv.at[it],
            device_id=other(j),
            device_id_type=MESH,
        )

    def scal_start(ref, send, recv, it):
        @pl.loop(1, n)
        def _(j):
            scal_copy(ref, send, recv, it, j).start()

    def scal_all(ref, send, recv, it):
        rest = ref.at[it, pl.ds(0, n - 1)]
        return pltpu.make_async_remote_copy(
            src_ref=rest,
            dst_ref=rest,
            send_sem=send.at[it],
            recv_sem=recv.at[it],
            device_id=other(1),
            device_id_type=MESH,
        )

    def total(x):
        return jnp.sum(jnp.sum(x, axis=0, keepdims=True), axis=1, keepdims=True)

    @pl.loop(0, tiles)
    def _(t):
        pltpu.make_async_copy(values_hbm.at[t], values.at[t], load_sem.at[t]).wait()
        alive = live(t)
        cols = jnp.sum(eye * (right_ref[pl.ds(t, 1), :] * alive), axis=1, keepdims=True)
        cols = jnp.broadcast_to(cols, (rows, LANES))
        for k in range(coupled):
            for h in range(halves):
                a = values[t, k, :, half(h)]
                terms[term_row(k, h, t), :] = jnp.sum(a * cols, axis=0, keepdims=True)
                squares[term_row(k, h, t), :] = (
                    jnp.sum(a * a, axis=0, keepdims=True) * alive
                )
        residual_ref[pl.ds(t, 1), :] = right_ref[pl.ds(t, 1), :] * alive

    pieces = scatter((terms, squares))
    for i in range(2):
        first_out[:, :, i] = pieces[i]
    pl.semaphore_wait(barrier, n - 1)
    first_copy = functools.partial(part_copy, first_out, first_in, first_send, first_recv)
    start_all(first_copy, True)
    first_in[own_slot] = first_out[own_rel, sub]
    wait_recv_all(first_copy, True)
    sums = jnp.sum(first_in[...], axis=0)
    normal_res = sums[0]
    jacobi = 1.0 / (1.0 + sums[1])
    scaled = jacobi * normal_res
    field_out[0] = scaled
    rho_part = total(normal_res * scaled)
    scal2[0, me] = jnp.broadcast_to(rho_part, (2, LANES))
    scal_start(scal2, scal2_send, scal2_recv, 0)
    start_all(functools.partial(field_copy, 0), False)
    field_in[0, own_rel, sub] = scaled
    wait_recv_all(functools.partial(field_copy, 0), False)
    scaled_win[...] = field_in[0].reshape(window, LANES)
    direction_win[...] = scaled_win[...]
    scal_all(scal2, scal2_send, scal2_recv, 0).wait_recv()
    rho_now = jnp.sum(scal2[0], axis=0)[0:1]

    answer = jnp.zeros((held, LANES), f32)
    own_rows = pl.ds(pl.multiple_of((n_sub + sub) * held, 8), held)
    for it in range(ITERS):
        last = it == ITERS - 1

        def tile_pass(t, norm):
            alive = live(t)
            m = None
            for k in range(coupled):
                for h in range(halves):
                    picked = direction_win[pl.ds(wid[t, k] + h * NB_DEV, 1), :] * alive
                    product = values[t, k, :, half(h)] * picked
                    m = product if m is None else m + product
            image = jnp.broadcast_to(jnp.sum(m, axis=1, keepdims=True), (rows, LANES))
            image_cols[t] = image
            if not last:
                for k in range(coupled):
                    for h in range(halves):
                        terms[term_row(k, h, t), :] = jnp.sum(
                            values[t, k, :, half(h)] * image, axis=0, keepdims=True
                        )
            return norm + jnp.sum(image * image, axis=0, keepdims=True)

        norm = lax.fori_loop(0, tiles, tile_pass, jnp.zeros((1, LANES), f32), unroll=2)
        scal1[it, me] = norm
        if not last:
            part_out[it] = scatter((terms,))[0]
            out_copy = functools.partial(
                part_copy, part_out.at[it], part_in.at[it], part_send.at[it], part_recv.at[it]
            )
            part_in[it, own_slot] = part_out[it, own_rel, sub]
            start_all(out_copy, True)
        scal_start(scal1, scal1_send, scal1_recv, it)

        @pl.loop(0, tiles)
        def _(t):
            image_rows[pl.ds(t, 1), :] = jnp.sum(image_cols[t] * eye, axis=0, keepdims=True)

        if not last:
            wait_recv_all(out_copy, True)
            back = jnp.sum(part_in[it], axis=0)
            back_scaled = jacobi * back
            field_out[it + 1] = back_scaled
            scal2[it + 1, me, 0:1] = jnp.broadcast_to(total(scaled * back), (1, LANES))
            scal2[it + 1, me, 1:2] = jnp.broadcast_to(total(back * back_scaled), (1, LANES))
            scal_start(scal2, scal2_send, scal2_recv, it + 1)
            start_all(functools.partial(field_copy, it + 1), False)
            field_in[it + 1, own_rel, sub] = back_scaled
        scal_all(scal1, scal1_send, scal1_recv, it).wait_recv()
        step_size = rho_now / jnp.sum(scal1[it], axis=0)
        answer = answer + step_size * direction_win[own_rows, :]
        residual_ref[...] = residual_ref[...] - step_size * image_rows[...]
        if not last:
            scaled = scaled - step_size * back_scaled
            wait_recv_all(functools.partial(field_copy, it + 1), False)
            scaled_win[...] = scaled_win[...] - step_size * field_in[it + 1].reshape(window, LANES)
            scal_all(scal2, scal2_send, scal2_recv, it + 1).wait_recv()
            both = jnp.sum(scal2[it + 1], axis=0)
            rho_next = rho_now - 2.0 * step_size * both[0:1] + step_size * step_size * both[1:2]
            direction_win[...] = scaled_win[...] + (rho_next / rho_now) * direction_win[...]
            rho_now = rho_next

    for h in range(halves):
        solution_ref[:, half(h)] = answer[h * NB_DEV : (h + 1) * NB_DEV]

    wait_send_all(first_copy, True)
    for it in range(ITERS):
        wait_send_all(functools.partial(field_copy, it), False)
        scal_all(scal1, scal1_send, scal1_recv, it).wait_send()
        scal_all(scal2, scal2_send, scal2_recv, it).wait_send()
        if it < ITERS - 1:
            wait_send_all(
                functools.partial(
                    part_copy, part_out.at[it], part_in.at[it], part_send.at[it], part_recv.at[it]
                ),
                True,
            )


def per_device(n_slab, n_sub, values, block_ids, tile_counts, right_side):
    tiles, coupled, rows, block = values.shape
    halves = block // LANES
    held = NB_DEV * halves
    n = n_slab * n_sub
    slots = 3 * n_sub
    window = slots * held
    n_terms = round_up(tiles * coupled * halves, LANES)
    n_window = round_up(window, LANES)
    f32 = jnp.float32
    vmem = pltpu.VMEM
    dma = pltpu.SemaphoreType.DMA
    whole = pl.BlockSpec(memory_space=pltpu.VMEM)
    return pl.pallas_call(
        functools.partial(kernel, n_slab, n_sub),
        out_shape=(
            jax.ShapeDtypeStruct((NB_DEV, block), f32),
            jax.ShapeDtypeStruct((tiles, rows), f32),
        ),
        in_specs=[pl.BlockSpec(memory_space=pl.ANY)] * 4,
        out_specs=(whole, whole),
        scratch_shapes=[
            vmem(values.shape, f32),
            pltpu.SMEM((tiles, coupled), jnp.int32),
            vmem((n_terms, n_window), f32),
            vmem((n_window, n_terms), jnp.bfloat16),
            vmem((n_terms, LANES), f32),
            vmem((n_terms, LANES), f32),
            vmem((tiles, rows, LANES), f32),
            vmem((tiles, LANES), f32),
            vmem((3, n_sub, 2, held, LANES), f32),
            vmem((slots, 2, held, LANES), f32),
            vmem((ITERS - 1, 3, n_sub, held, LANES), f32),
            vmem((ITERS - 1, slots, held, LANES), f32),
            vmem((ITERS, held, LANES), f32),
            vmem((ITERS, 3, n_sub, held, LANES), f32),
            vmem((window, LANES), f32),
            vmem((window, LANES), f32),
            vmem((ITERS, n, 1, LANES), f32),
            vmem((ITERS, n, 2, LANES), f32),
            pltpu.SMEM((tiles, coupled), jnp.int32),
            pltpu.SMEM((1, 1), jnp.int32),
            vmem((tiles, rows), f32),
            dma((3,)),
            dma((tiles,)),
            dma((slots,)),
            dma((slots,)),
            dma((ITERS - 1, slots)),
            dma((ITERS - 1, slots)),
            dma((ITERS, slots)),
            dma((ITERS, slots)),
            dma((ITERS,)),
            dma((ITERS,)),
            dma((ITERS,)),
            dma((ITERS,)),
        ],
        compiler_params=pltpu.CompilerParams(
            collective_id=0, has_side_effects=True, vmem_limit_bytes=48 * 1024 * 1024
        ),
    )(values, block_ids, tile_counts, right_side)


def solution(mesh):
    in_specs = (
        P(("slab", "sub"), None, None, None),
        P(("slab", "sub"), None),
        P("slab", "sub"),
        P(("slab", "sub"), None),
    )
    out_specs = (P(("slab", "sub"), None), P(("slab", "sub"), None))
    return jax.shard_map(
        functools.partial(per_device, mesh.shape["slab"], mesh.shape["sub"]),
        mesh=mesh,
        in_specs=in_specs,
        out_specs=out_specs,
        check_vma=False,
    )
```

```python
import functools

import jax
import jax.numpy as jnp
from jax import lax
from jax.experimental import pallas as pl
from jax.experimental.pallas import tpu as pltpu
from jax.sharding import PartitionSpec as P

ITERS = 4
NB_DEV = 12
LANES = 128
MESH = pl.DeviceIdType.MESH


def round_up(size, unit):
    return -(-size // unit) * unit


def kernel(
    n_slab,
    n_sub,
    values_hbm,
    ids_hbm,
    counts_hbm,
    right_hbm,
    solution_ref,
    residual_ref,
    values,
    wid,
    turned,
    selector,
    terms,
    squares,
    image_cols,
    image_rows,
    first_out,
    first_in,
    part_out,
    part_in,
    field_out,
    field_in,
    field_win,
    scal1,
    scal2,
    ids_smem,
    counts_smem,
    right_ref,
    small_sem,
    load_sem,
    first_send,
    first_recv,
    part_send,
    part_recv,
    field_send,
    field_recv,
    scal1_send,
    scal1_recv,
    scal2_send,
    scal2_recv,
):
    tiles, coupled, rows, block = values.shape
    halves = block // LANES
    held = NB_DEV * halves
    n = n_slab * n_sub
    window = 3 * n_sub * held
    f32 = jnp.float32
    slab = lax.axis_index("slab")
    sub = lax.axis_index("sub")
    me = slab * n_sub + sub

    def keeper(s):
        return s + 1 - 2 * lax.rem(s, 2) if n_slab % 2 == 0 else s

    kept = keeper(slab)

    small = [
        pltpu.make_async_copy(src, dst, small_sem.at[i])
        for i, (src, dst) in enumerate(
            ((ids_hbm, ids_smem), (counts_hbm, counts_smem), (right_hbm, right_ref))
        )
    ]
    for copy in small:
        copy.start()
    for t in range(tiles):
        pltpu.make_async_copy(values_hbm.at[t], values.at[t], load_sem.at[t]).start()

    def other(j):
        target = lax.rem(me + j, n)
        return (lax.div(target, n_sub), lax.rem(target, n_sub))

    barrier = pltpu.get_barrier_semaphore()

    @pl.loop(1, n)
    def _(j):
        pl.semaphore_signal(barrier, inc=1, device_id=other(j), device_id_type=MESH)

    for copy in small:
        copy.wait()

    turned[...] = jnp.zeros_like(turned)
    terms[...] = jnp.zeros_like(terms)
    squares[...] = jnp.zeros_like(squares)
    lane_ids = lax.broadcasted_iota(jnp.int32, (1, turned.shape[1]), 1)

    @pl.loop(0, tiles)
    def _(t):
        for k in range(coupled):
            b = ids_smem[t, k]
            owner = lax.div(b, NB_DEV)
            rel = jnp.clip(lax.div(owner, n_sub) - slab + 1, 0, 2)
            row = (rel * n_sub + lax.rem(owner, n_sub)) * held + lax.rem(b, NB_DEV)
            wid[t, k] = row
            for h in range(halves):
                hot = (lane_ids == row + h * NB_DEV).astype(f32)
                turned[pl.ds((k * halves + h) * tiles + t, 1), :] = hot

    selector[...] = turned[...].T.astype(jnp.bfloat16)

    def blank_part(low):
        first_in[low : low + n_sub] = jnp.zeros((n_sub,) + first_in.shape[1:], f32)
        for it in range(part_in.shape[0]):
            part_in[it, low : low + n_sub] = jnp.zeros((n_sub,) + part_in.shape[2:], f32)

    def blank_field(rel):
        for it in range(field_in.shape[0]):
            field_in[it, rel] = jnp.zeros(field_in.shape[2:], f32)

    pl.when(kept == 0)(lambda: blank_part(2 * n_sub))
    pl.when(kept == n_slab - 1)(lambda: blank_part(0))
    pl.when(slab == 0)(lambda: blank_field(0))
    pl.when(slab == n_slab - 1)(lambda: blank_field(2))

    def live(t):
        return jnp.where(t < counts_smem[0, 0], 1.0, 0.0).astype(f32)

    eye = (
        lax.broadcasted_iota(jnp.int32, (rows, LANES), 0)
        == lax.broadcasted_iota(jnp.int32, (rows, LANES), 1)
    ).astype(f32)

    def half(h):
        return slice(h * LANES, (h + 1) * LANES)

    def term_row(k, h, t):
        return pl.ds((k * halves + h) * tiles + t, 1)

    def scatter(term_refs):
        cut = []
        for ref in term_refs:
            rest = ref[...]
            for _ in range(3):
                piece = rest.astype(jnp.bfloat16)
                cut.append(piece)
                rest = rest - piece.astype(f32)
        spread = jnp.dot(
            selector[...], jnp.concatenate(cut, axis=1), preferred_element_type=f32
        )
        outs = []
        for i in range(len(term_refs)):
            a, b, c = (spread[:window, half(3 * i + j)] for j in range(3))
            outs.append((a + (b + c)).reshape(3, n_sub, held, LANES))
        return outs

    def inside(s):
        return jnp.logical_and(s >= 0, s < n_slab)

    def each(act, scatters):
        for ds in (1, -1, 0):
            for step in range(n_sub):
                if scatters:
                    exists, far = inside(slab + ds), keeper(slab + ds)
                else:
                    exists, far = inside(kept - ds), kept - ds
                if step == 0:
                    exists = jnp.logical_and(exists, far != slab)
                pl.when(exists)(functools.partial(act, ds, step))

    def part_copy(out_ref, in_ref, send, recv, ds, step):
        target = lax.rem(sub + step, n_sub)
        slot = (ds + 1) * n_sub + step
        return pltpu.make_async_remote_copy(
            src_ref=out_ref.at[ds + 1, target],
            dst_ref=in_ref.at[slot],
            send_sem=send.at[slot],
            recv_sem=recv.at[slot],
            device_id=(keeper(slab + ds), target),
            device_id_type=MESH,
        )

    def field_copy(it, ds, step):
        target = lax.rem(sub + step, n_sub)
        slot = (ds + 1) * n_sub + step
        return pltpu.make_async_remote_copy(
            src_ref=field_out.at[it],
            dst_ref=field_in.at[it, ds + 1, sub],
            send_sem=field_send.at[it, slot],
            recv_sem=field_recv.at[it, slot],
            device_id=(kept - ds, target),
            device_id_type=MESH,
        )

    def start_all(copy, scatters):
        each(lambda ds, step: copy(ds, step).start(), scatters)

    def wait_recv_all(copy, scatters):
        each(lambda ds, step: copy(ds, step).wait_recv(), not scatters)

    def wait_send_all(copy, scatters):
        each(lambda ds, step: copy(ds, step).wait_send(), scatters)

    own_rel = kept - slab + 1
    own_slot = own_rel * n_sub

    def scal_copy(ref, send, recv, it, j):
        return pltpu.make_async_remote_copy(
            src_ref=ref.at[it, me],
            dst_ref=ref.at[it, me],
            send_sem=send.at[it],
            recv_sem=recv.at[it],
            device_id=other(j),
            device_id_type=MESH,
        )

    def scal_start(ref, send, recv, it):
        @pl.loop(1, n)
        def _(j):
            scal_copy(ref, send, recv, it, j).start()

    def scal_all(ref, send, recv, it):
        rest = ref.at[it, pl.ds(0, n - 1)]
        return pltpu.make_async_remote_copy(
            src_ref=rest,
            dst_ref=rest,
            send_sem=send.at[it],
            recv_sem=recv.at[it],
            device_id=other(1),
            device_id_type=MESH,
        )

    def total(x):
        return jnp.sum(jnp.sum(x, axis=0, keepdims=True), axis=1, keepdims=True)

    @pl.loop(0, tiles)
    def _(t):
        pltpu.make_async_copy(values_hbm.at[t], values.at[t], load_sem.at[t]).wait()
        alive = live(t)
        cols = jnp.sum(eye * (right_ref[pl.ds(t, 1), :] * alive), axis=1, keepdims=True)
        cols = jnp.broadcast_to(cols, (rows, LANES))
        for k in range(coupled):
            for h in range(halves):
                a = values[t, k, :, half(h)]
                terms[term_row(k, h, t), :] = jnp.sum(a * cols, axis=0, keepdims=True)
                squares[term_row(k, h, t), :] = (
                    jnp.sum(a * a, axis=0, keepdims=True) * alive
                )
        residual_ref[pl.ds(t, 1), :] = right_ref[pl.ds(t, 1), :] * alive

    pieces = scatter((terms, squares))
    for i in range(2):
        first_out[:, :, i] = pieces[i]
    pl.semaphore_wait(barrier, n - 1)
    first_copy = functools.partial(part_copy, first_out, first_in, first_send, first_recv)
    start_all(first_copy, True)
    first_in[own_slot] = first_out[own_rel, sub]
    wait_recv_all(first_copy, True)
    sums = jnp.sum(first_in[...], axis=0)
    normal_res = sums[0]
    jacobi = 1.0 / (1.0 + sums[1])
    scaled = jacobi * normal_res
    field_out[0] = scaled
    rho_part = total(normal_res * scaled)
    scal2[0, me] = jnp.broadcast_to(rho_part, (2, LANES))
    start_all(functools.partial(field_copy, 0), False)
    scal_start(scal2, scal2_send, scal2_recv, 0)
    field_in[0, own_rel, sub] = scaled
    wait_recv_all(functools.partial(field_copy, 0), False)
    answer = jnp.zeros((held, LANES), f32)
    for it in range(ITERS):
        last = it == ITERS - 1
        field_win[...] = field_in[it].reshape(window, LANES)

        def tile_pass(t, carry):
            alive = live(t)
            m = None
            for k in range(coupled):
                for h in range(halves):
                    picked = field_win[pl.ds(wid[t, k] + h * NB_DEV, 1), :] * alive
                    product = values[t, k, :, half(h)] * picked
                    m = product if m is None else m + product
            image = jnp.broadcast_to(jnp.sum(m, axis=1, keepdims=True), (rows, LANES))
            image_cols[t] = image
            if not last:
                for k in range(coupled):
                    for h in range(halves):
                        terms[term_row(k, h, t), :] = jnp.sum(
                            values[t, k, :, half(h)] * image, axis=0, keepdims=True
                        )
            return carry

        lax.fori_loop(0, tiles, tile_pass, 0, unroll=8)
        if not last:
            part_out[it] = scatter((terms,))[0]
            out_copy = functools.partial(
                part_copy, part_out.at[it], part_in.at[it], part_send.at[it], part_recv.at[it]
            )
            part_in[it, own_slot] = part_out[it, own_rel, sub]
            start_all(out_copy, True)

        @pl.loop(0, tiles, unroll=4)
        def _(t):
            image_rows[pl.ds(t, 1), :] = jnp.sum(image_cols[t] * eye, axis=0, keepdims=True)

        field_own = field_in[it, 1, sub]
        if it == 0:
            scal_all(scal2, scal2_send, scal2_recv, 0).wait_recv()
            rho_now = jnp.sum(scal2[0], axis=0)[0:1]
            scaled_own = field_own
            direction = field_own
            scaled_image = image_rows[...]
            image = scaled_image
        else:
            scal_all(scal1, scal1_send, scal1_recv, it - 1).wait_recv()
            step_size = rho_now / jnp.sum(scal1[it - 1], axis=0)
            answer = answer + step_size * direction
            residual_ref[...] = residual_ref[...] - step_size * image
            scaled = scaled - step_size * back_scaled
            scal_all(scal2, scal2_send, scal2_recv, it).wait_recv()
            both = jnp.sum(scal2[it], axis=0)
            rho_next = rho_now - 2.0 * step_size * both[0:1] + step_size * step_size * both[1:2]
            beta = rho_next / rho_now
            rho_now = rho_next
            scaled_own = scaled_own - step_size * field_own
            direction = scaled_own + beta * direction
            scaled_image = scaled_image - step_size * image_rows[...]
            image = scaled_image + beta * image
        scal1[it, me] = jnp.broadcast_to(total(image * image), (1, LANES))
        scal_start(scal1, scal1_send, scal1_recv, it)

        if not last:
            wait_recv_all(out_copy, True)
            spread = jnp.sum(part_in[it], axis=0)
            if it == 0:
                scaled_back = spread
                back = spread
            else:
                scaled_back = scaled_back - step_size * spread
                back = scaled_back + beta * back
            back_scaled = jacobi * back
            field_out[it + 1] = back_scaled
            start_all(functools.partial(field_copy, it + 1), False)
            scal2[it + 1, me, 0:1] = jnp.broadcast_to(total(scaled * back), (1, LANES))
            scal2[it + 1, me, 1:2] = jnp.broadcast_to(total(back * back_scaled), (1, LANES))
            scal_start(scal2, scal2_send, scal2_recv, it + 1)
            field_in[it + 1, own_rel, sub] = back_scaled
            wait_recv_all(functools.partial(field_copy, it + 1), False)

    scal_all(scal1, scal1_send, scal1_recv, ITERS - 1).wait_recv()
    step_size = rho_now / jnp.sum(scal1[ITERS - 1], axis=0)
    answer = answer + step_size * direction
    residual_ref[...] = residual_ref[...] - step_size * image
    for h in range(halves):
        solution_ref[:, half(h)] = answer[h * NB_DEV : (h + 1) * NB_DEV]

    wait_send_all(first_copy, True)
    for it in range(ITERS):
        wait_send_all(functools.partial(field_copy, it), False)
        scal_all(scal1, scal1_send, scal1_recv, it).wait_send()
        scal_all(scal2, scal2_send, scal2_recv, it).wait_send()
        if it < ITERS - 1:
            wait_send_all(
                functools.partial(
                    part_copy, part_out.at[it], part_in.at[it], part_send.at[it], part_recv.at[it]
                ),
                True,
            )


def per_device(n_slab, n_sub, values, block_ids, tile_counts, right_side):
    tiles, coupled, rows, block = values.shape
    halves = block // LANES
    held = NB_DEV * halves
    n = n_slab * n_sub
    slots = 3 * n_sub
    window = slots * held
    n_terms = round_up(tiles * coupled * halves, LANES)
    n_window = round_up(window, LANES)
    f32 = jnp.float32
    vmem = pltpu.VMEM
    dma = pltpu.SemaphoreType.DMA
    whole = pl.BlockSpec(memory_space=pltpu.VMEM)
    return pl.pallas_call(
        functools.partial(kernel, n_slab, n_sub),
        out_shape=(
            jax.ShapeDtypeStruct((NB_DEV, block), f32),
            jax.ShapeDtypeStruct((tiles, rows), f32),
        ),
        in_specs=[pl.BlockSpec(memory_space=pl.ANY)] * 4,
        out_specs=(whole, whole),
        scratch_shapes=[
            vmem(values.shape, f32),
            pltpu.SMEM((tiles, coupled), jnp.int32),
            vmem((n_terms, n_window), f32),
            vmem((n_window, n_terms), jnp.bfloat16),
            vmem((n_terms, LANES), f32),
            vmem((n_terms, LANES), f32),
            vmem((tiles, rows, LANES), f32),
            vmem((tiles, LANES), f32),
            vmem((3, n_sub, 2, held, LANES), f32),
            vmem((slots, 2, held, LANES), f32),
            vmem((ITERS - 1, 3, n_sub, held, LANES), f32),
            vmem((ITERS - 1, slots, held, LANES), f32),
            vmem((ITERS, held, LANES), f32),
            vmem((ITERS, 3, n_sub, held, LANES), f32),
            vmem((window, LANES), f32),
            vmem((ITERS, n, 1, LANES), f32),
            vmem((ITERS, n, 2, LANES), f32),
            pltpu.SMEM((tiles, coupled), jnp.int32),
            pltpu.SMEM((1, 1), jnp.int32),
            vmem((tiles, rows), f32),
            dma((3,)),
            dma((tiles,)),
            dma((slots,)),
            dma((slots,)),
            dma((ITERS - 1, slots)),
            dma((ITERS - 1, slots)),
            dma((ITERS, slots)),
            dma((ITERS, slots)),
            dma((ITERS,)),
            dma((ITERS,)),
            dma((ITERS,)),
            dma((ITERS,)),
        ],
        compiler_params=pltpu.CompilerParams(
            collective_id=0, has_side_effects=True, vmem_limit_bytes=48 * 1024 * 1024
        ),
    )(values, block_ids, tile_counts, right_side)


def solution(mesh):
    in_specs = (
        P(("slab", "sub"), None, None, None),
        P(("slab", "sub"), None),
        P("slab", "sub"),
        P(("slab", "sub"), None),
    )
    out_specs = (P(("slab", "sub"), None), P(("slab", "sub"), None))
    return jax.shard_map(
        functools.partial(per_device, mesh.shape["slab"], mesh.shape["sub"]),
        mesh=mesh,
        in_specs=in_specs,
        out_specs=out_specs,
        check_vma=False,
    )
```

```python
import functools

import jax
import jax.numpy as jnp
from jax import lax
from jax.experimental import pallas as pl
from jax.experimental.pallas import tpu as pltpu
from jax.sharding import PartitionSpec as P

ITERS = 4
NB_DEV = 12
LANES = 128
MESH = pl.DeviceIdType.MESH


def round_up(size, unit):
    return -(-size // unit) * unit


def kernel(
    n_slab,
    n_sub,
    values_hbm,
    ids_hbm,
    counts_hbm,
    right_hbm,
    solution_ref,
    residual_ref,
    values,
    wid,
    turned,
    selector,
    terms,
    squares,
    image_cols,
    image_rows,
    first_out,
    first_in,
    part_out,
    part_in,
    field_out,
    field_in,
    field_win,
    scal1,
    scal2,
    ids_smem,
    counts_smem,
    right_ref,
    small_sem,
    load_sem,
    first_send,
    first_recv,
    part_send,
    part_recv,
    field_send,
    field_recv,
    scal1_send,
    scal1_recv,
    scal2_send,
    scal2_recv,
):
    tiles, coupled, rows, block = values.shape
    halves = block // LANES
    held = NB_DEV * halves
    n = n_slab * n_sub
    window = 3 * n_sub * held
    f32 = jnp.float32
    slab = lax.axis_index("slab")
    sub = lax.axis_index("sub")
    me = slab * n_sub + sub

    def keeper(s):
        return s + 1 - 2 * lax.rem(s, 2) if n_slab % 2 == 0 else s

    kept = keeper(slab)

    small = [
        pltpu.make_async_copy(src, dst, small_sem.at[i])
        for i, (src, dst) in enumerate(
            ((ids_hbm, ids_smem), (counts_hbm, counts_smem), (right_hbm, right_ref))
        )
    ]
    for copy in small:
        copy.start()
    for t in range(tiles):
        pltpu.make_async_copy(values_hbm.at[t], values.at[t], load_sem.at[t]).start()

    def other(j):
        target = lax.rem(me + j, n)
        return (lax.div(target, n_sub), lax.rem(target, n_sub))

    barrier = pltpu.get_barrier_semaphore()

    @pl.loop(1, n)
    def _(j):
        pl.semaphore_signal(barrier, inc=1, device_id=other(j), device_id_type=MESH)

    for copy in small:
        copy.wait()

    turned[...] = jnp.zeros_like(turned)
    terms[...] = jnp.zeros_like(terms)
    squares[...] = jnp.zeros_like(squares)
    lane_ids = lax.broadcasted_iota(jnp.int32, (1, turned.shape[1]), 1)

    @pl.loop(0, tiles)
    def _(t):
        for k in range(coupled):
            b = ids_smem[t, k]
            owner = lax.div(b, NB_DEV)
            rel = jnp.clip(lax.div(owner, n_sub) - slab + 1, 0, 2)
            row = (rel * n_sub + lax.rem(owner, n_sub)) * held + lax.rem(b, NB_DEV)
            wid[t, k] = row
            for h in range(halves):
                hot = (lane_ids == row + h * NB_DEV).astype(f32)
                turned[pl.ds((k * halves + h) * tiles + t, 1), :] = hot

    selector[...] = turned[...].T.astype(jnp.bfloat16)

    def blank_part(low):
        first_in[low : low + n_sub] = jnp.zeros((n_sub,) + first_in.shape[1:], f32)
        for it in range(part_in.shape[0]):
            part_in[it, low : low + n_sub] = jnp.zeros((n_sub,) + part_in.shape[2:], f32)

    def blank_field(rel):
        for it in range(field_in.shape[0]):
            field_in[it, rel] = jnp.zeros(field_in.shape[2:], f32)

    pl.when(kept == 0)(lambda: blank_part(2 * n_sub))
    pl.when(kept == n_slab - 1)(lambda: blank_part(0))
    pl.when(slab == 0)(lambda: blank_field(0))
    pl.when(slab == n_slab - 1)(lambda: blank_field(2))

    def live(t):
        return jnp.where(t < counts_smem[0, 0], 1.0, 0.0).astype(f32)

    eye = (
        lax.broadcasted_iota(jnp.int32, (rows, LANES), 0)
        == lax.broadcasted_iota(jnp.int32, (rows, LANES), 1)
    ).astype(f32)

    def half(h):
        return slice(h * LANES, (h + 1) * LANES)

    def term_row(k, h, t):
        return pl.ds((k * halves + h) * tiles + t, 1)

    def scatter(term_refs):
        cut = []
        for ref in term_refs:
            rest = ref[...]
            for _ in range(3):
                piece = rest.astype(jnp.bfloat16)
                cut.append(piece)
                rest = rest - piece.astype(f32)
        spread = jnp.dot(
            selector[...], jnp.concatenate(cut, axis=1), preferred_element_type=f32
        )
        outs = []
        for i in range(len(term_refs)):
            a, b, c = (spread[:window, half(3 * i + j)] for j in range(3))
            outs.append((a + (b + c)).reshape(3, n_sub, held, LANES))
        return outs

    def inside(s):
        return jnp.logical_and(s >= 0, s < n_slab)

    def each(act, scatters):
        for ds in (1, -1, 0):
            for step in (*range(1, n_sub), 0):
                if scatters:
                    exists, far = inside(slab + ds), keeper(slab + ds)
                else:
                    exists, far = inside(kept - ds), kept - ds
                if step == 0:
                    exists = jnp.logical_and(exists, far != slab)
                pl.when(exists)(functools.partial(act, ds, step))

    def part_copy(out_ref, in_ref, send, recv, ds, step):
        target = lax.rem(sub + step, n_sub)
        slot = (ds + 1) * n_sub + step
        return pltpu.make_async_remote_copy(
            src_ref=out_ref.at[ds + 1, target],
            dst_ref=in_ref.at[slot],
            send_sem=send.at[slot],
            recv_sem=recv.at[slot],
            device_id=(keeper(slab + ds), target),
            device_id_type=MESH,
        )

    def field_copy(it, ds, step):
        target = lax.rem(sub + step, n_sub)
        slot = (ds + 1) * n_sub + step
        return pltpu.make_async_remote_copy(
            src_ref=field_out.at[it],
            dst_ref=field_in.at[it, ds + 1, sub],
            send_sem=field_send.at[it, slot],
            recv_sem=field_recv.at[it, slot],
            device_id=(kept - ds, target),
            device_id_type=MESH,
        )

    def start_all(copy, scatters):
        each(lambda ds, step: copy(ds, step).start(), scatters)

    def wait_recv_all(copy, scatters):
        each(lambda ds, step: copy(ds, step).wait_recv(), not scatters)

    def wait_send_all(copy, scatters):
        each(lambda ds, step: copy(ds, step).wait_send(), scatters)

    own_rel = kept - slab + 1
    own_slot = own_rel * n_sub

    def scal_copy(ref, send, recv, it, j):
        return pltpu.make_async_remote_copy(
            src_ref=ref.at[it, me],
            dst_ref=ref.at[it, me],
            send_sem=send.at[it],
            recv_sem=recv.at[it],
            device_id=other(j),
            device_id_type=MESH,
        )

    def scal_start(ref, send, recv, it):
        @pl.loop(1, n)
        def _(j):
            scal_copy(ref, send, recv, it, j).start()

    def scal_all(ref, send, recv, it):
        rest = ref.at[it, pl.ds(0, n - 1)]
        return pltpu.make_async_remote_copy(
            src_ref=rest,
            dst_ref=rest,
            send_sem=send.at[it],
            recv_sem=recv.at[it],
            device_id=other(1),
            device_id_type=MESH,
        )

    def total(x):
        return jnp.sum(jnp.sum(x, axis=0, keepdims=True), axis=1, keepdims=True)

    @pl.loop(0, tiles)
    def _(t):
        pltpu.make_async_copy(values_hbm.at[t], values.at[t], load_sem.at[t]).wait()
        alive = live(t)
        cols = jnp.sum(eye * (right_ref[pl.ds(t, 1), :] * alive), axis=1, keepdims=True)
        cols = jnp.broadcast_to(cols, (rows, LANES))
        for k in range(coupled):
            for h in range(halves):
                a = values[t, k, :, half(h)]
                terms[term_row(k, h, t), :] = jnp.sum(a * cols, axis=0, keepdims=True)
                squares[term_row(k, h, t), :] = (
                    jnp.sum(a * a, axis=0, keepdims=True) * alive
                )
        residual_ref[pl.ds(t, 1), :] = right_ref[pl.ds(t, 1), :] * alive

    pieces = scatter((terms, squares))
    for i in range(2):
        first_out[:, :, i] = pieces[i]
    pl.semaphore_wait(barrier, n - 1)
    first_copy = functools.partial(part_copy, first_out, first_in, first_send, first_recv)
    start_all(first_copy, True)
    first_in[own_slot] = first_out[own_rel, sub]
    wait_recv_all(first_copy, True)
    sums = jnp.sum(first_in[...], axis=0)
    normal_res = sums[0]
    jacobi = 1.0 / (1.0 + sums[1])
    scaled = jacobi * normal_res
    field_out[0] = scaled
    rho_part = total(normal_res * scaled)
    scal2[0, me] = jnp.broadcast_to(rho_part, (2, LANES))
    start_all(functools.partial(field_copy, 0), False)
    scal_start(scal2, scal2_send, scal2_recv, 0)
    field_in[0, own_rel, sub] = scaled
    wait_recv_all(functools.partial(field_copy, 0), False)
    answer = jnp.zeros((held, LANES), f32)
    for it in range(ITERS):
        last = it == ITERS - 1
        field_win[...] = field_in[it].reshape(window, LANES)

        def tile_pass(t, carry):
            alive = live(t)
            m = None
            for k in range(coupled):
                for h in range(halves):
                    picked = field_win[pl.ds(wid[t, k] + h * NB_DEV, 1), :] * alive
                    product = values[t, k, :, half(h)] * picked
                    m = product if m is None else m + product
            image = jnp.broadcast_to(jnp.sum(m, axis=1, keepdims=True), (rows, LANES))
            image_cols[t] = image
            if not last:
                for k in range(coupled):
                    for h in range(halves):
                        terms[term_row(k, h, t), :] = jnp.sum(
                            values[t, k, :, half(h)] * image, axis=0, keepdims=True
                        )
            return carry

        lax.fori_loop(0, tiles, tile_pass, 0, unroll=8)
        if not last:
            part_out[it] = scatter((terms,))[0]
            out_copy = functools.partial(
                part_copy, part_out.at[it], part_in.at[it], part_send.at[it], part_recv.at[it]
            )
            part_in[it, own_slot] = part_out[it, own_rel, sub]
            start_all(out_copy, True)

        @pl.loop(0, tiles, unroll=4)
        def _(t):
            image_rows[pl.ds(t, 1), :] = jnp.sum(image_cols[t] * eye, axis=0, keepdims=True)

        field_own = field_in[it, 1, sub]
        if it == 0:
            scal_all(scal2, scal2_send, scal2_recv, 0).wait_recv()
            rho_now = jnp.sum(scal2[0], axis=0)[0:1]
            scaled_own = field_own
            direction = field_own
            scaled_image = image_rows[...]
            image = scaled_image
        else:
            scal_all(scal1, scal1_send, scal1_recv, it - 1).wait_recv()
            step_size = rho_now / jnp.sum(scal1[it - 1], axis=0)
            answer = answer + step_size * direction
            residual_ref[...] = residual_ref[...] - step_size * image
            scaled = scaled - step_size * back_scaled
            scal_all(scal2, scal2_send, scal2_recv, it).wait_recv()
            both = jnp.sum(scal2[it], axis=0)
            rho_next = rho_now - 2.0 * step_size * both[0:1] + step_size * step_size * both[1:2]
            beta = rho_next / rho_now
            rho_now = rho_next
            scaled_own = scaled_own - step_size * field_own
            direction = scaled_own + beta * direction
            scaled_image = scaled_image - step_size * image_rows[...]
            image = scaled_image + beta * image
        scal1[it, me] = jnp.broadcast_to(total(image * image), (1, LANES))
        scal_start(scal1, scal1_send, scal1_recv, it)

        if not last:
            wait_recv_all(out_copy, True)
            spread = jnp.sum(part_in[it], axis=0)
            if it == 0:
                scaled_back = spread
                back = spread
            else:
                scaled_back = scaled_back - step_size * spread
                back = scaled_back + beta * back
            back_scaled = jacobi * back
            field_out[it + 1] = back_scaled
            start_all(functools.partial(field_copy, it + 1), False)
            scal2[it + 1, me, 0:1] = jnp.broadcast_to(total(scaled * back), (1, LANES))
            scal2[it + 1, me, 1:2] = jnp.broadcast_to(total(back * back_scaled), (1, LANES))
            scal_start(scal2, scal2_send, scal2_recv, it + 1)
            field_in[it + 1, own_rel, sub] = back_scaled
            wait_recv_all(functools.partial(field_copy, it + 1), False)

    scal_all(scal1, scal1_send, scal1_recv, ITERS - 1).wait_recv()
    step_size = rho_now / jnp.sum(scal1[ITERS - 1], axis=0)
    answer = answer + step_size * direction
    residual_ref[...] = residual_ref[...] - step_size * image
    for h in range(halves):
        solution_ref[:, half(h)] = answer[h * NB_DEV : (h + 1) * NB_DEV]

    wait_send_all(first_copy, True)
    for it in range(ITERS):
        wait_send_all(functools.partial(field_copy, it), False)
        scal_all(scal1, scal1_send, scal1_recv, it).wait_send()
        scal_all(scal2, scal2_send, scal2_recv, it).wait_send()
        if it < ITERS - 1:
            wait_send_all(
                functools.partial(
                    part_copy, part_out.at[it], part_in.at[it], part_send.at[it], part_recv.at[it]
                ),
                True,
            )


def per_device(n_slab, n_sub, values, block_ids, tile_counts, right_side):
    tiles, coupled, rows, block = values.shape
    halves = block // LANES
    held = NB_DEV * halves
    n = n_slab * n_sub
    slots = 3 * n_sub
    window = slots * held
    n_terms = round_up(tiles * coupled * halves, LANES)
    n_window = round_up(window, LANES)
    f32 = jnp.float32
    vmem = pltpu.VMEM
    dma = pltpu.SemaphoreType.DMA
    whole = pl.BlockSpec(memory_space=pltpu.VMEM)
    return pl.pallas_call(
        functools.partial(kernel, n_slab, n_sub),
        out_shape=(
            jax.ShapeDtypeStruct((NB_DEV, block), f32),
            jax.ShapeDtypeStruct((tiles, rows), f32),
        ),
        in_specs=[pl.BlockSpec(memory_space=pl.ANY)] * 4,
        out_specs=(whole, whole),
        scratch_shapes=[
            vmem(values.shape, f32),
            pltpu.SMEM((tiles, coupled), jnp.int32),
            vmem((n_terms, n_window), f32),
            vmem((n_window, n_terms), jnp.bfloat16),
            vmem((n_terms, LANES), f32),
            vmem((n_terms, LANES), f32),
            vmem((tiles, rows, LANES), f32),
            vmem((tiles, LANES), f32),
            vmem((3, n_sub, 2, held, LANES), f32),
            vmem((slots, 2, held, LANES), f32),
            vmem((ITERS - 1, 3, n_sub, held, LANES), f32),
            vmem((ITERS - 1, slots, held, LANES), f32),
            vmem((ITERS, held, LANES), f32),
            vmem((ITERS, 3, n_sub, held, LANES), f32),
            vmem((window, LANES), f32),
            vmem((ITERS, n, 1, LANES), f32),
            vmem((ITERS, n, 2, LANES), f32),
            pltpu.SMEM((tiles, coupled), jnp.int32),
            pltpu.SMEM((1, 1), jnp.int32),
            vmem((tiles, rows), f32),
            dma((3,)),
            dma((tiles,)),
            dma((slots,)),
            dma((slots,)),
            dma((ITERS - 1, slots)),
            dma((ITERS - 1, slots)),
            dma((ITERS, slots)),
            dma((ITERS, slots)),
            dma((ITERS,)),
            dma((ITERS,)),
            dma((ITERS,)),
            dma((ITERS,)),
        ],
        compiler_params=pltpu.CompilerParams(
            collective_id=0, has_side_effects=True, vmem_limit_bytes=48 * 1024 * 1024
        ),
    )(values, block_ids, tile_counts, right_side)


def solution(mesh):
    in_specs = (
        P(("slab", "sub"), None, None, None),
        P(("slab", "sub"), None),
        P("slab", "sub"),
        P(("slab", "sub"), None),
    )
    out_specs = (P(("slab", "sub"), None), P(("slab", "sub"), None))
    return jax.shard_map(
        functools.partial(per_device, mesh.shape["slab"], mesh.shape["sub"]),
        mesh=mesh,
        in_specs=in_specs,
        out_specs=out_specs,
        check_vma=False,
    )
```
